128 devices in a mesh: data: 1, tp: 16 (over z, y), ep: 8 (over x, core).
Axes of the slice: x: 4, y: 4, z: 4, core: 2. Of those that a mesh axis runs over, the one named last changes fastest.
Arguments:
- tokens_a: bfloat16 [32768, 1280], P(('data', 'ep', 'tp'))
- tokens_b: bfloat16 [32768, 1280], P(('data', 'ep', 'tp'))
- experts_a: int32 [32768, 6], P(('data', 'ep', 'tp'))
- experts_b: int32 [32768, 6], P(('data', 'ep', 'tp'))
- gates_a: float32 [32768, 6], P(('data', 'ep', 'tp'))
- gates_b: float32 [32768, 6], P(('data', 'ep', 'tp'))
- slots_a: int32 [32768, 6], P(('data', 'ep', 'tp'))
- slots_b: int32 [32768, 6], P(('data', 'ep', 'tp'))
- shared_w1: bfloat16 [1280, 1792], P(None, 'tp')
- shared_w3: bfloat16 [1280, 1792], P(None, 'tp')
- shared_w2: bfloat16 [1792, 1280], P('tp')
- routed_w1: bfloat16 [64, 1280, 896], P('ep')
- routed_w3: bfloat16 [64, 1280, 896], P('ep')
- routed_w2: bfloat16 [64, 896, 1280], P('ep')
Outputs:
- output 1: bfloat16 [32768, 1280], P(('data', 'ep', 'tp'))
- output 2: bfloat16 [32768, 1280], P(('data', 'ep', 'tp'))
All inputs are finite; a program needn't handle non-finite values.
Results may differ from the reference program's by a relative error of at most 0.00503706.
Values are sent between devices in bfloat16 or wider.
A program may use at most 1 GiB of HBM per device.

```python
import jax
import jax.numpy as jnp
from jax import lax

TOK_DEV = 256
TP_SIZE = 16
EP_SIZE = 8
MODEL_DIM = 1280
EXPERTS = 64
TOP_K = 6
EXPERT_FF = 896
SHARED_FF = 1792
CAPACITY = 48

GROUP_DEVS = TP_SIZE * EP_SIZE
GROUP_TOK = GROUP_DEVS * TOK_DEV


def draw_routing(key):
    key_base, key_rank, key_tie = jax.random.split(key, 3)
    base = jax.random.randint(key_base, (GROUP_TOK, EXPERTS), 0, 64)
    rank_of = jax.random.permutation(key_rank, EXPERTS)
    favoured = jnp.where((rank_of >= 1) & (rank_of <= EXPERTS // 8), 6, 0)
    forced = jnp.where(rank_of == 0, 4096, 0)
    tok_ids = jnp.arange(GROUP_TOK)
    head_tok = (tok_ids % TOK_DEV) < CAPACITY
    cover = jnp.where(tok_ids[:, None] == jnp.arange(EXPERTS)[None, :], 4096, 0)
    score = base + favoured[None, :] + jnp.where(head_tok[:, None], forced[None, :], 0) + cover
    tie_rank = jax.random.permutation(key_tie, jnp.broadcast_to(jnp.arange(EXPERTS), (GROUP_TOK, EXPERTS)), axis=1, independent=True)
    chosen = lax.top_k(score * EXPERTS + tie_rank, TOP_K)[1]
    per_dev = chosen.reshape(GROUP_DEVS, TOK_DEV * TOP_K)
    one_hot = (per_dev[:, :, None] == jnp.arange(EXPERTS)[None, None, :]).astype(jnp.int32)
    earlier = jnp.cumsum(one_hot, axis=1) - one_hot
    position = jnp.sum(earlier * one_hot, axis=2)
    slots = jnp.where(position < CAPACITY, position, -1).reshape(GROUP_TOK, TOP_K)
    return chosen.astype(jnp.int32), slots.astype(jnp.int32)


def setup_inputs(seed: int = 0, part: int = 0) -> dict:
    key = jax.random.key(seed)
    part_keys = jax.random.split(jax.random.fold_in(key, part), 6)
    weight_keys = jax.random.split(key, 6)
    tokens_a = jax.random.normal(part_keys[0], (GROUP_TOK, MODEL_DIM), jnp.float32).astype(jnp.bfloat16)
    tokens_b = jax.random.normal(part_keys[1], (GROUP_TOK, MODEL_DIM), jnp.float32).astype(jnp.bfloat16)
    experts_a, slots_a = draw_routing(part_keys[2])
    experts_b, slots_b = draw_routing(part_keys[3])
    gates_a = jax.random.uniform(part_keys[4], (GROUP_TOK, TOP_K), jnp.float32, 0.5, 1.5) * TOP_K ** -0.5
    gates_b = jax.random.uniform(part_keys[5], (GROUP_TOK, TOP_K), jnp.float32, 0.5, 1.5) * TOP_K ** -0.5
    shared_w1 = (jax.random.normal(weight_keys[0], (MODEL_DIM, SHARED_FF), jnp.float32) * MODEL_DIM ** -0.5).astype(jnp.bfloat16)
    shared_w3 = (jax.random.normal(weight_keys[1], (MODEL_DIM, SHARED_FF), jnp.float32) * MODEL_DIM ** -0.5).astype(jnp.bfloat16)
    shared_w2 = (jax.random.normal(weight_keys[2], (SHARED_FF, MODEL_DIM), jnp.float32) * SHARED_FF ** -0.5).astype(jnp.bfloat16)
    routed_w1 = (jax.random.normal(weight_keys[3], (EXPERTS, MODEL_DIM, EXPERT_FF), jnp.float32) * MODEL_DIM ** -0.5).astype(jnp.bfloat16)
    routed_w3 = (jax.random.normal(weight_keys[4], (EXPERTS, MODEL_DIM, EXPERT_FF), jnp.float32) * MODEL_DIM ** -0.5).astype(jnp.bfloat16)
    routed_w2 = (jax.random.normal(weight_keys[5], (EXPERTS, EXPERT_FF, MODEL_DIM), jnp.float32) * EXPERT_FF ** -0.5).astype(jnp.bfloat16)
    return {'tokens_a': tokens_a, 'tokens_b': tokens_b, 'experts_a': experts_a, 'experts_b': experts_b, 'gates_a': gates_a, 'gates_b': gates_b, 'slots_a': slots_a, 'slots_b': slots_b, 'shared_w1': shared_w1, 'shared_w3': shared_w3, 'shared_w2': shared_w2, 'routed_w1': routed_w1, 'routed_w3': routed_w3, 'routed_w2': routed_w2}


def swiglu_rows(rows, w_in, w_gate, w_out):
    proj_in = jnp.dot(rows, w_in, preferred_element_type=jnp.float32)
    proj_gate = jnp.dot(rows, w_gate, preferred_element_type=jnp.float32)
    hidden = (jax.nn.silu(proj_in) * proj_gate).astype(jnp.bfloat16)
    return jnp.dot(hidden, w_out, preferred_element_type=jnp.float32)


def shared_expert(tokens, shared_w1, shared_w3, shared_w2):
    blocks = tokens.reshape(GROUP_DEVS, TOK_DEV, MODEL_DIM)
    result = lax.map(lambda token_block: swiglu_rows(token_block, shared_w1, shared_w3, shared_w2), blocks)
    return result.reshape(GROUP_TOK, MODEL_DIM)


def routed_experts(tokens, experts, gates, slots, routed_w1, routed_w3, routed_w2):
    tok_dev = tokens.reshape(GROUP_DEVS, TOK_DEV, MODEL_DIM).astype(jnp.float32)
    expert_dev = experts.reshape(GROUP_DEVS, TOK_DEV, TOP_K)
    slot_dev = slots.reshape(GROUP_DEVS, TOK_DEV, TOP_K)
    gate_dev = gates.reshape(GROUP_DEVS, TOK_DEV, TOP_K)
    slot_range = jnp.arange(CAPACITY)

    def one_expert(routed_acc, step_in):
        w_in, w_gate, w_out, expert = step_in
        hits = ((expert_dev == expert)[..., None] & (slot_dev[..., None] == slot_range)).astype(jnp.float32)
        place_mat = jnp.sum(hits, axis=2)
        gate_mat = jnp.sum(hits * gate_dev[..., None], axis=2)
        buffer_rows = jnp.einsum('ntc,ntd->ncd', place_mat, tok_dev).astype(jnp.bfloat16)
        expert_out = swiglu_rows(buffer_rows.reshape(GROUP_DEVS * CAPACITY, MODEL_DIM), w_in, w_gate, w_out).astype(jnp.bfloat16)
        expert_out = expert_out.reshape(GROUP_DEVS, CAPACITY, MODEL_DIM).astype(jnp.float32)
        return routed_acc + jnp.einsum('ntc,ncd->ntd', gate_mat, expert_out), None

    start_acc = jnp.zeros((GROUP_DEVS, TOK_DEV, MODEL_DIM), jnp.float32)
    routed_acc, unused = lax.scan(one_expert, start_acc, (routed_w1, routed_w3, routed_w2, jnp.arange(EXPERTS)))
    return routed_acc.reshape(GROUP_TOK, MODEL_DIM)


def one_microbatch(tokens, experts, gates, slots, shared_w1, shared_w3, shared_w2, routed_w1, routed_w3, routed_w2):
    shared_out = shared_expert(tokens, shared_w1, shared_w3, shared_w2)
    routed_out = routed_experts(tokens, experts, gates, slots, routed_w1, routed_w3, routed_w2)
    return (tokens.astype(jnp.float32) + shared_out + routed_out).astype(jnp.bfloat16)


def reference(tokens_a, tokens_b, experts_a, experts_b, gates_a, gates_b, slots_a, slots_b, shared_w1, shared_w3, shared_w2, routed_w1, routed_w3, routed_w2):
    out_a = one_microbatch(tokens_a, experts_a, gates_a, slots_a, shared_w1, shared_w3, shared_w2, routed_w1, routed_w3, routed_w2)
    out_b = one_microbatch(tokens_b, experts_b, gates_b, slots_b, shared_w1, shared_w3, shared_w2, routed_w1, routed_w3, routed_w2)
    return (out_a, out_b)
```

```python
import jax
import jax.numpy as jnp
from jax import lax
from jax.sharding import PartitionSpec as P


def split_gate(gate):
    high = lax.reduce_precision(gate, 8, 7)
    rest = gate - high
    middle = lax.reduce_precision(rest, 8, 7)
    low = rest - middle
    return [part.astype(jnp.bfloat16) for part in (high, middle, low)]


def solution(mesh):
    ep_size = mesh.shape['ep']
    tok_spec = P(('data', 'ep', 'tp'), None)
    in_specs = (tok_spec,) * 8 + (P(None, 'tp'), P(None, 'tp'), P('tp', None), P('ep', None, None), P('ep', None, None), P('ep', None, None))

    def layer_local(tokens_a, tokens_b, experts_a, experts_b, gates_a, gates_b, slots_a, slots_b, shared_w1, shared_w3, shared_w2, routed_w1, routed_w3, routed_w2):
        tok_local, top_k = experts_a.shape
        local_experts, model_dim, expert_ff = routed_w1.shape
        num_experts = local_experts * ep_size
        cap = max(4, (2 * tok_local * top_k) // num_experts)
        rows = local_experts * cap
        rank = lax.axis_index('ep')

        def row_of(experts, slots):
            return jnp.where(slots >= 0, experts * cap + slots, -1).astype(jnp.float32)

        meta = jnp.concatenate([row_of(experts_a, slots_a), row_of(experts_b, slots_b), gates_a, gates_b], axis=1)
        meta = lax.all_gather(meta, 'ep', axis=0)
        first_row = (rank * rows).astype(jnp.float32)
        gathered_a = lax.all_gather(tokens_a, 'ep', axis=0)
        gathered_b = lax.all_gather(tokens_b, 'ep', axis=0)
        w1t = lax.all_gather(shared_w1.T, 'tp', axis=0, tiled=True)
        w3t = lax.all_gather(shared_w3.T, 'tp', axis=0, tiled=True)
        w2 = lax.all_gather(shared_w2, 'tp', axis=0, tiled=True)

        def routed(gathered, row_ids, gates):
            local_row = row_ids - first_row
            hits = local_row[:, :, :, None] == jnp.arange(rows, dtype=jnp.float32)
            place = jnp.any(hits, axis=2).astype(jnp.bfloat16)
            gate_mat = jnp.sum(jnp.where(hits, gates[:, :, :, None], 0.0), axis=2)
            place = place.reshape(ep_size, tok_local, local_experts, cap)
            recv = jnp.einsum('stec,std->escd', place, gathered, preferred_element_type=jnp.float32).astype(jnp.bfloat16)
            recv = recv.reshape(local_experts, ep_size * cap, model_dim)
            proj_in = jnp.einsum('erd,edf->erf', recv, routed_w1, preferred_element_type=jnp.float32)
            proj_gate = jnp.einsum('erd,edf->erf', recv, routed_w3, preferred_element_type=jnp.float32)
            hidden = (jax.nn.silu(proj_in) * proj_gate).astype(jnp.bfloat16)
            result = jnp.einsum('erf,efd->erd', hidden, routed_w2, preferred_element_type=jnp.float32).astype(jnp.bfloat16)
            result = result.reshape(local_experts, ep_size, cap, model_dim)
            partial = 0.0
            for part in split_gate(gate_mat):
                part = part.reshape(ep_size, tok_local, local_experts, cap)
                partial = partial + jnp.einsum('stec,escd->std', part, result, preferred_element_type=jnp.float32)
            return lax.psum_scatter(partial, 'ep', scatter_dimension=0, tiled=False)

        def shared(x_local):
            dims = (((1,), (1,)), ((), ()))
            proj_in = lax.dot_general(x_local, w1t, dims, preferred_element_type=jnp.float32)
            proj_gate = lax.dot_general(x_local, w3t, dims, preferred_element_type=jnp.float32)
            hidden = (jax.nn.silu(proj_in) * proj_gate).astype(jnp.bfloat16)
            return jnp.dot(hidden, w2, preferred_element_type=jnp.float32)

        row_a, row_b, gate_a, gate_b = (meta[:, :, top_k * i:top_k * (i + 1)] for i in range(4))
        routed_a = routed(gathered_a, row_a, gate_a)
        routed_b = routed(gathered_b, row_b, gate_b)
        out_a = (tokens_a.astype(jnp.float32) + shared(tokens_a) + routed_a).astype(jnp.bfloat16)
        out_b = (tokens_b.astype(jnp.float32) + shared(tokens_b) + routed_b).astype(jnp.bfloat16)
        return (out_a, out_b)

    return jax.shard_map(layer_local, mesh=mesh, in_specs=in_specs, out_specs=(tok_spec, tok_spec), check_vma=False)
```

```python
import functools

import jax
import jax.numpy as jnp
from jax import lax
from jax.experimental import pallas as pl
from jax.experimental.pallas import tpu as pltpu
from jax.sharding import PartitionSpec as P

MESH = pl.DeviceIdType.MESH
F32 = jnp.float32
BF16 = jnp.bfloat16


def _split_gate(gate):
    high = gate.astype(BF16)
    rest = gate - high.astype(F32)
    middle = rest.astype(BF16)
    low = (rest - middle.astype(F32)).astype(BF16)
    return high, middle, low


def _layer_kernel(
    cap, top_k,
    tok_a, tok_b, meta_in, shared_in, routed_w1, routed_w3, routed_w2,
    out_a, out_b, far_hbm, gath_hbm,
    near, stage, meta, rows, w13, w2, hid, pair_out, pair_in, sums, turn_p, turn_m, last_p, last_m,
    sem_near, sem_near_recv, sem_meta_send, sem_meta_recv, sem_ag_send, sem_ag_recv, sem_stage, sem_w,
    sem_sh_send, sem_sh_recv, sem_sh_own, sem_sh_load, sem_pair_send, sem_pair_recv, sem_rs_send, sem_rs_recv, pair_free,
):
    local_experts, model_dim, ff = routed_w1.shape
    tok = tok_a.shape[0]
    half = tok // 2
    shard = shared_in.shape[1]
    num_rows = local_experts * cap
    tile = 256
    n_tiles = model_dim // tile
    f_tiles = ff // 128

    ep = lax.axis_index('ep')
    tp = lax.axis_index('tp')
    chip, core = ep // 2, lax.rem(ep, 2)
    z, y = tp // 4, lax.rem(tp, 4)

    def on_x(step, other=0):
        side = core if other == 0 else 1 - core
        return {'ep': lax.rem(chip + step, 4) * 2 + side, 'tp': tp}

    def on_y(step):
        return {'ep': ep, 'tp': z * 4 + lax.rem(y + step, 4)}

    def on_z(step):
        return {'ep': ep, 'tp': lax.rem(z + step, 4) * 4 + y}

    def remote(src, dst, send, recv, device):
        return pltpu.make_async_remote_copy(src_ref=src, dst_ref=dst, send_sem=send, recv_sem=recv, device_id=device, device_id_type=MESH)

    low, high = pl.ds(0, half), pl.ds(half, half)

    tokens = (tok_a, tok_b)

    def ag_own(m, k):
        part, step, slot = ((low, 1, 6), (high, 1, 6), (high, 3, 2), (low, 3, 2))[k]
        return remote(tokens[m].at[part], far_hbm.at[m, slot, part], sem_ag_send.at[m, k], sem_ag_recv.at[m, k], on_x(step))

    def ag_relay(m, k):
        part, step, slot = ((low, 1, 6), (high, 3, 2))[k]
        return remote(far_hbm.at[m, slot, part], far_hbm.at[m, 4, part], sem_ag_send.at[m, 4 + k], sem_ag_recv.at[m, 4 + k], on_x(step))

    def ag_pair(m, k):
        slot = (6, 2, 4)[k]
        return remote(far_hbm.at[m, slot], far_hbm.at[m, slot + 1], sem_ag_send.at[m, 6 + k], sem_ag_recv.at[m, 6 + k], on_x(0, 1))

    def near_pair(m):
        return remote(tokens[m], near.at[2 * m + 1], sem_near.at[m], sem_near_recv.at[m], on_x(0, 1))

    def near_own(m):
        return pltpu.make_async_copy(tokens[m], near.at[2 * m], sem_near.at[2 + m])

    def meta_send(dx, other):
        back = (4 - dx) % 4
        slot = back * 2 + other
        return remote(meta_in, meta.at[slot], sem_meta_send.at[dx * 2 + other], sem_meta_recv.at[slot], on_x(dx, other))

    meta_own = pltpu.make_async_copy(meta_in, meta.at[0], sem_meta_send.at[0])
    others = [(dx, other) for dx in range(4) for other in range(2) if (dx, other) != (0, 0)]

    mine = lax.rem(y, 2) == core
    own_slot = z * 2 + y // 2

    def shard_y(k):
        return remote(shared_in, gath_hbm.at[own_slot], sem_sh_send.at[k], sem_sh_recv.at[own_slot], on_y((1, 3, 2)[k]))

    shard_own = pltpu.make_async_copy(shared_in, gath_hbm.at[own_slot], sem_sh_own)

    def shard_wait(slot):
        pltpu.make_async_copy(shared_in, gath_hbm.at[slot], sem_sh_recv.at[slot]).wait()

    def shard_z(k):
        slot = z * 2 + k % 2
        return remote(gath_hbm.at[slot], gath_hbm.at[slot], sem_sh_send.at[3 + k], sem_sh_recv.at[slot], on_z((1, 3)[k // 2]))

    def shard_relay(k):
        slot = lax.rem(z + (3, 1)[k], 4) * 2 + k
        return remote(gath_hbm.at[slot], gath_hbm.at[slot], sem_sh_send.at[7 + k], sem_sh_recv.at[slot], on_z((1, 3)[k]))

    def weights(buf, expert, act):
        for j in range(f_tiles):
            col = pl.ds(128 * j, 128)
            act(pltpu.make_async_copy(routed_w1.at[expert, :, col], w13.at[buf, j, :, pl.ds(0, 128)], sem_w.at[buf, 2 * j]))
            act(pltpu.make_async_copy(routed_w3.at[expert, :, col], w13.at[buf, j, :, pl.ds(128, 128)], sem_w.at[buf, 2 * j + 1]))
        act(pltpu.make_async_copy(routed_w2.at[expert], w2.at[buf], sem_w.at[buf, 2 * f_tiles]))

    def pair_copy(n):
        k = lax.rem(n, 2)
        return remote(pair_out.at[k], pair_in.at[k], sem_pair_send.at[n], sem_pair_recv.at[n], on_x(0, 1))

    def rs_turn(m, k):
        part, step, dst = ((low, 1, turn_p), (high, 3, turn_m))[k]
        return remote(sums.at[m, 0, part], dst.at[m], sem_rs_send.at[m, k], sem_rs_recv.at[m, k], on_x(step))

    def rs_last(m, k):
        part, step, dst, i = ((high, 1, last_m, 1), (low, 3, last_p, 2), (low, 1, last_m, 1), (high, 3, last_p, 2))[k]
        return remote(sums.at[m, i, part], dst.at[m, part], sem_rs_send.at[m, 2 + k], sem_rs_recv.at[m, 2 + k], on_x(step))

    def hits_of(slot, m):
        ids = meta[slot, 2 * m] - (ep * num_rows).astype(F32)
        row = lax.broadcasted_iota(jnp.int32, (num_rows, tok), 0).astype(F32)
        return [row == ids[j:j + 1, :] for j in range(top_k)]

    def place(q, slot, m, src, src_index):
        hits = hits_of(slot, m)
        matrix = functools.reduce(jnp.logical_or, hits)
        matrix = jnp.where(matrix, 1.0, 0.0).astype(BF16)
        for n in range(n_tiles):
            col = pl.ds(n * tile, tile)
            picked = jnp.dot(matrix, src[src_index, :, col], preferred_element_type=F32).astype(BF16)
            rows[:, q, :, col] = picked.reshape(local_experts, cap, tile)

    def ffn(expert, count, q0, nq):
        buf = lax.rem(count, 2)
        weights(buf, expert, lambda c: c.wait())

        @pl.when(count + 1 < 3 * local_experts)
        def _():
            weights(1 - buf, lax.rem(expert + 1, local_experts), lambda c: c.start())

        size = nq * cap
        x = rows[expert, pl.ds(q0, nq)].reshape(size, model_dim)
        for j in range(f_tiles):
            both = jnp.dot(x, w13[buf, j], preferred_element_type=F32)
            hid[pl.ds(0, size), pl.ds(128 * j, 128)] = (jax.nn.silu(both[:, :128]) * both[:, 128:]).astype(BF16)
        h = hid[pl.ds(0, size), :]
        for n in range(n_tiles):
            col = pl.ds(n * tile, tile)
            res = jnp.dot(h, w2[buf, :, col], preferred_element_type=F32).astype(BF16)
            rows[expert, pl.ds(q0, nq), :, col] = res.reshape(nq, cap, tile)

    def combine(q, slot, m, dst, add):
        gates = meta[slot, 2 * m + 1]
        matrix = 0.0
        for j, hit in enumerate(hits_of(slot, m)):
            matrix = matrix + jnp.where(hit, gates[j:j + 1, :], 0.0)
        matrix = jnp.concatenate(_split_gate(matrix), axis=0)
        for n in range(n_tiles):
            col = pl.ds(n * tile, tile)
            res = rows[:, q, :, col].reshape(num_rows, tile)
            res = jnp.concatenate([res, res, res], axis=0)
            part = lax.dot_general(matrix, res, (((0,), (0,)), ((), ())), preferred_element_type=F32)
            dst[:, col] = dst[:, col] + part if add else part

    def add_into(dst, src):
        step = min(32, dst.shape[0])

        def body(i, carry):
            part = pl.ds(pl.multiple_of(i * step, step), step)
            dst[part, :] = dst[part, :] + src[part, :]
            return carry
        lax.fori_loop(0, dst.shape[0] // step, body, 0)

    def shared(q, dst):
        x = near[q]
        width = min(tile, ff)
        dims = (((1,), (1,)), ((), ()))
        for start in range(0, ff, width):
            size = min(width, ff - start)
            row = pl.ds(start, size)
            a = lax.dot_general(x, w2[0, row, :], dims, preferred_element_type=F32)
            g = lax.dot_general(x, w2[1, row, :], dims, preferred_element_type=F32)
            hid[pl.ds(0, tok), row] = (jax.nn.silu(a) * g).astype(BF16)
        h = hid[pl.ds(0, tok), :]
        for n in range(n_tiles):
            dst[:, pl.ds(n * tile, tile)] = jnp.dot(h, w13[0, n, pl.ds(0, ff), :], preferred_element_type=F32)

    def shared_load(act):
        def body(k, carry):
            row = pl.ds(pl.multiple_of(k * shard, shard), shard)
            act(pltpu.make_async_copy(gath_hbm.at[k, 0], w2.at[0, row], sem_sh_load.at[k, 0]))
            act(pltpu.make_async_copy(gath_hbm.at[k, 1], w2.at[1, row], sem_sh_load.at[k, 1]))
            for n in range(n_tiles):
                act(pltpu.make_async_copy(gath_hbm.at[k, 2, :, pl.ds(n * tile, tile)], w13.at[0, n, row], sem_sh_load.at[k, 2 + n]))
            return carry
        lax.fori_loop(0, 8, body, 0)

    weights(0, 0, lambda c: c.start())
    near_own(0).start()
    near_own(1).start()
    meta_own.start()
    barrier = pltpu.get_barrier_semaphore()
    peers = [on_x(dx, other) for dx, other in others] + [on_y(1), on_y(2), on_y(3), on_z(1), on_z(3)]
    for peer in peers:
        pl.semaphore_signal(barrier, inc=1, device_id=peer, device_id_type=MESH)
    pl.semaphore_wait(barrier, len(peers))

    for k in (0, 2, 1, 3):
        ag_own(0, k).start()
    near_pair(0).start()
    near_pair(1).start()
    for dx, other in others:
        meta_send(dx, other).start()

    @pl.when(mine)
    def _():
        for k in range(3):
            shard_y(k).start()
        shard_own.start()

    meta_own.wait()
    near_own(0).wait()
    near_own(1).wait()
    near_pair(0).wait_recv()
    near_pair(1).wait_recv()
    meta_send(0, 1).wait_recv()

    def place_near(q, carry):
        place(q, lax.rem(q, 2), q // 2, near, q)
        return carry
    lax.fori_loop(0, 4, place_near, 0)

    def ffn_near(e, carry):
        @pl.when(e == 2)
        def _():
            ag_own(0, 0).wait_recv()
            ag_relay(0, 0).start()
            ag_own(0, 2).wait_recv()
            ag_relay(0, 1).start()
            for k in (0, 2, 1, 3):
                ag_own(1, k).start()

        @pl.when(e == 5)
        def _():
            ag_own(0, 1).wait_recv()
            ag_pair(0, 0).start()
            ag_own(0, 3).wait_recv()
            ag_pair(0, 1).start()

        @pl.when(e == 7)
        def _():
            for h in range(2):
                owned = jnp.logical_and(mine, y // 2 == h)

                @pl.when(owned)
                def _():
                    shard_own.wait()

                @pl.when(jnp.logical_not(owned))
                def _():
                    shard_wait(z * 2 + h)
            for k in range(4):
                shard_z(k).start()
        ffn(e, e, 0, 4)
        return carry
    lax.fori_loop(0, local_experts, ffn_near, 0)

    for dx, other in others[1:]:
        meta_send(dx, other).wait_recv()
    ag_relay(0, 0).wait_recv()
    ag_relay(0, 1).wait_recv()
    ag_pair(0, 2).start()

    def turn(m):
        rs_turn(m, 0).wait_recv()
        add_into(sums.at[m, 1, low], turn_p.at[m])
        rs_last(m, 2).start()
        rs_turn(m, 1).wait_recv()
        add_into(sums.at[m, 2, high], turn_m.at[m])
        rs_last(m, 3).start()

    def stage_copy(m, i):
        k = lax.rem(i, 2)
        return pltpu.make_async_copy(far_hbm.at[m, i + 2], stage.at[k], sem_stage.at[k])

    def far(m, carry):
        for k in range(3):
            ag_pair(m, k).wait_recv()
        stage_copy(m, 0).start()

        def place_far(i, carry):
            stage_copy(m, i).wait()

            @pl.when(i < 5)
            def _():
                stage_copy(m, i + 1).start()
            place(4 + 6 * m + i, 2 + i, m, stage, lax.rem(i, 2))
            return carry
        lax.fori_loop(0, 6, place_far, 0)

        def ffn_far(e, carry):
            @pl.when(jnp.logical_and(m == 0, e == 1))
            def _():
                ag_own(1, 0).wait_recv()
                ag_relay(1, 0).start()
                ag_own(1, 2).wait_recv()
                ag_relay(1, 1).start()

            @pl.when(jnp.logical_and(m == 0, e == 4))
            def _():
                ag_own(1, 1).wait_recv()
                ag_pair(1, 0).start()
                ag_own(1, 3).wait_recv()
                ag_pair(1, 1).start()

            @pl.when(jnp.logical_and(m == 0, e == 7))
            def _():
                ag_relay(1, 0).wait_recv()
                ag_relay(1, 1).wait_recv()
                ag_pair(1, 2).start()

            @pl.when(jnp.logical_and(m == 1, e == 0))
            def _():
                for step in (1, 3):
                    for h in range(2):
                        shard_wait(lax.rem(z + step, 4) * 2 + h)
                for k in range(2):
                    shard_relay(k).start()

            @pl.when(jnp.logical_and(m == 1, e == 4))
            def _():
                turn(0)
            ffn(e, local_experts * (1 + m) + e, 4 + 6 * m, 6)
            return carry
        lax.fori_loop(0, local_experts, ffn_far, 0)

        @pl.when(m == 1)
        def _():
            for h in range(2):
                shard_wait(lax.rem(z + 2, 4) * 2 + h)
            shared_load(lambda c: c.start())

        def combine_far(i, carry):
            n = 3 * m + i
            k = lax.rem(n, 2)
            slot = 3 * i * i - 5 * i + 4

            @pl.when(n >= 2)
            def _():
                pair_copy(n - 2).wait_send()
            combine(2 + 6 * m + slot + 1, slot + 1, m, pair_out.at[k], False)

            @pl.when(n >= 2)
            def _():
                pl.semaphore_wait(pair_free, 1)
            pair_copy(n).start()
            combine(2 + 6 * m + slot, slot, m, sums.at[m, i], False)
            pair_copy(n).wait_recv()
            add_into(sums.at[m, i], pair_in.at[k])
            pl.semaphore_signal(pair_free, inc=1, device_id=on_x(0, 1), device_id_type=MESH)

            @pl.when(i == 0)
            def _():
                rs_turn(m, 0).start()
                rs_turn(m, 1).start()

            @pl.when(i == 1)
            def _():
                rs_last(m, 0).start()

            @pl.when(i == 2)
            def _():
                rs_last(m, 1).start()
            return carry
        lax.fori_loop(0, 3, combine_far, 0)
        return carry

    lax.fori_loop(0, 2, far, 0)

    shared_load(lambda c: c.wait())

    def finish(m, carry):
        n = 6 + m
        k = lax.rem(n, 2)
        pair_copy(n - 2).wait_send()
        shared(2 * m + 1, pair_out.at[k])
        combine(2 * m + 1, 1, m, pair_out.at[k], True)
        pl.semaphore_wait(pair_free, 1)
        pair_copy(n).start()
        shared(2 * m, sums.at[m, 3])
        combine(2 * m, 0, m, sums.at[m, 3], True)

        @pl.when(m == 0)
        def _():
            turn(1)
        pair_copy(n).wait_recv()
        add_into(sums.at[m, 3], pair_in.at[k])
        return carry
    lax.fori_loop(0, 2, finish, 0)

    step = min(32, tok)
    for m, out in enumerate((out_a, out_b)):
        for k in (0, 2, 1, 3):
            rs_last(m, k).wait_recv()

        def write(i, carry):
            part = pl.ds(pl.multiple_of(i * step, step), step)
            total = near[2 * m, part, :].astype(F32) + sums[m, 3, part, :]
            out[part, :] = (total + last_p[m, part, :] + last_m[m, part, :]).astype(BF16)
            return carry
        lax.fori_loop(0, tok // step, write, 0)

    for m in range(2):
        for k in range(4):
            ag_own(m, k).wait_send()
            rs_last(m, k).wait_send()
        for k in range(2):
            ag_relay(m, k).wait_send()
            rs_turn(m, k).wait_send()
        for k in range(3):
            ag_pair(m, k).wait_send()
        near_pair(m).wait_send()
        pair_copy(6 + m).wait_send()
    for dx, other in others:
        meta_send(dx, other).wait_send()

    @pl.when(mine)
    def _():
        for k in range(3):
            shard_y(k).wait_send()
    for k in range(4):
        shard_z(k).wait_send()
    for k in range(2):
        shard_relay(k).wait_send()


def solution(mesh):
    ep_size = mesh.shape['ep']
    tok_spec = P(('data', 'ep', 'tp'), None)
    in_specs = (tok_spec,) * 8 + (P(None, 'tp'), P(None, 'tp'), P('tp', None), P('ep', None, None), P('ep', None, None), P('ep', None, None))

    def layer_local(tokens_a, tokens_b, experts_a, experts_b, gates_a, gates_b, slots_a, slots_b, shared_w1, shared_w3, shared_w2, routed_w1, routed_w3, routed_w2):
        tok, top_k = experts_a.shape
        local_experts, model_dim, ff = routed_w1.shape
        shard = shared_w2.shape[0]
        cap = max(4, (2 * tok * top_k) // (local_experts * ep_size))
        half = tok // 2
        f_tiles, n_tiles = ff // 128, model_dim // 256

        def row_of(experts, slots):
            return jnp.where(slots >= 0, experts * cap + slots, -1).astype(F32)

        meta = jnp.stack([row_of(experts_a, slots_a), gates_a, row_of(experts_b, slots_b), gates_b])
        meta = jnp.pad(meta.transpose(0, 2, 1), ((0, 0), (0, 8 - top_k), (0, 0)))
        shared_in = jnp.stack([shared_w1.T, shared_w3.T, shared_w2])

        hbm = pl.BlockSpec(memory_space=pl.ANY)
        vmem = pl.BlockSpec(memory_space=pltpu.VMEM)
        dma = pltpu.SemaphoreType.DMA
        row_count = local_experts * cap * ep_size
        flops = 2 * row_count * model_dim * ff * 6 + 4 * tok * model_dim * ff * 6
        out_a, out_b, _, _ = pl.pallas_call(
            functools.partial(_layer_kernel, cap, top_k),
            out_shape=(
                jax.ShapeDtypeStruct((tok, model_dim), BF16),
                jax.ShapeDtypeStruct((tok, model_dim), BF16),
                jax.ShapeDtypeStruct((2, 8, tok, model_dim), BF16),
                jax.ShapeDtypeStruct((8, 3, shard, model_dim), BF16),
            ),
            in_specs=[hbm] * 7,
            out_specs=(vmem, vmem, hbm, hbm),
            scratch_shapes=[
                pltpu.VMEM((4, tok, model_dim), BF16),
                pltpu.VMEM((2, tok, model_dim), BF16),
                pltpu.VMEM((8, 4, 8, tok), F32),
                pltpu.VMEM((local_experts, 16, cap, model_dim), BF16),
                pltpu.VMEM((2, f_tiles, model_dim, 256), BF16),
                pltpu.VMEM((2, ff, model_dim), BF16),
                pltpu.VMEM((max(6 * cap, tok), ff), BF16),
                pltpu.VMEM((2, tok, model_dim), F32),
                pltpu.VMEM((2, tok, model_dim), F32),
                pltpu.VMEM((2, 4, tok, model_dim), F32),
                pltpu.VMEM((2, half, model_dim), F32),
                pltpu.VMEM((2, half, model_dim), F32),
                pltpu.VMEM((2, tok, model_dim), F32),
                pltpu.VMEM((2, tok, model_dim), F32),
                dma((4,)), dma((2,)), dma((8,)), dma((8,)), dma((2, 9)), dma((2, 9)), dma((2,)), dma((2, 2 * f_tiles + 1)),
                dma((9,)), dma((8,)), dma, dma((8, 2 + n_tiles)), dma((8,)), dma((8,)), dma((2, 6)), dma((2, 6)),
                pltpu.SemaphoreType.REGULAR,
            ],
            compiler_params=pltpu.CompilerParams(collective_id=0, has_side_effects=True, vmem_limit_bytes=67_000_000),
            cost_estimate=pl.CostEstimate(flops=flops, bytes_accessed=200_000_000, transcendentals=0),
        )(tokens_a, tokens_b, meta, shared_in, routed_w1, routed_w3, routed_w2)
        return (out_a, out_b)

    return jax.shard_map(layer_local, mesh=mesh, in_specs=in_specs, out_specs=(tok_spec, tok_spec), check_vma=False)
```

```python
import functools

import jax
import jax.numpy as jnp
from jax import lax
from jax.experimental import pallas as pl
from jax.experimental.pallas import tpu as pltpu
from jax.sharding import PartitionSpec as P

MESH = pl.DeviceIdType.MESH
F32 = jnp.float32
BF16 = jnp.bfloat16
ORDER = (0, 2, 1, 3)


def _split_gate(gate):
    high = gate.astype(BF16)
    rest = gate - high.astype(F32)
    middle = rest.astype(BF16)
    low = (rest - middle.astype(F32)).astype(BF16)
    return high, middle, low


def _layer_kernel(
    cap, top_k,
    tok_a, tok_b, exp_a, exp_b, gate_a, gate_b, slot_a, slot_b, shared_w1, shared_w3, shared_w2, routed_w1, routed_w3, routed_w2,
    out_a, out_b, far_hbm, gath_hbm,
    near, stage, meta, rows, w1, w3, w2, hid, pair_out, pair_in, sums, turn_p, turn_m, last_p, last_m, shard_vmem,
    sem_near, sem_near_recv, sem_meta_send, sem_meta_recv, sem_ag_send, sem_ag_recv, sem_stage, sem_w,
    sem_sh_send, sem_sh_recv, sem_sh_own, sem_sh_load, sem_pair_send, sem_pair_recv, sem_rs_send, sem_rs_recv, sem_out, pair_free,
):
    local_experts, model_dim, ff = routed_w1.shape
    tok = tok_a.shape[0]
    half = tok // 2
    shard = shared_w2.shape[0]
    num_rows = local_experts * cap
    tile = 256
    n_tiles = model_dim // tile
    f_tiles = ff // 128

    ep = lax.axis_index('ep')
    tp = lax.axis_index('tp')
    chip, core = ep // 2, lax.rem(ep, 2)
    z, y = tp // 4, lax.rem(tp, 4)

    def on_x(step, other=0):
        side = core if other == 0 else 1 - core
        return {'ep': lax.rem(chip + step, 4) * 2 + side, 'tp': tp}

    def on_y(step):
        return {'ep': ep, 'tp': z * 4 + lax.rem(y + step, 4)}

    def on_z(step):
        return {'ep': ep, 'tp': lax.rem(z + step, 4) * 4 + y}

    def remote(src, dst, send, recv, device):
        return pltpu.make_async_remote_copy(src_ref=src, dst_ref=dst, send_sem=send, recv_sem=recv, device_id=device, device_id_type=MESH)

    low, high = pl.ds(0, half), pl.ds(half, half)

    tokens = (tok_a, tok_b)

    def ag_own(m, k):
        part, step, slot = ((low, 1, 6), (high, 1, 6), (high, 3, 2), (low, 3, 2))[k]
        return remote(tokens[m].at[part], far_hbm.at[m, slot, part], sem_ag_send.at[m, k], sem_ag_recv.at[m, k], on_x(step))

    def ag_relay(m, k):
        part, step, slot = ((low, 1, 6), (high, 3, 2))[k]
        return remote(far_hbm.at[m, slot, part], far_hbm.at[m, 4, part], sem_ag_send.at[m, 4 + k], sem_ag_recv.at[m, 4 + k], on_x(step))

    def ag_pair(m, k):
        slot = (6, 2, 4)[k]
        return remote(far_hbm.at[m, slot], far_hbm.at[m, slot + 1], sem_ag_send.at[m, 6 + k], sem_ag_recv.at[m, 6 + k], on_x(0, 1))

    def near_pair(m):
        return remote(tokens[m], near.at[2 * m + 1], sem_near.at[m], sem_near_recv.at[m], on_x(0, 1))

    def near_own(m):
        return pltpu.make_async_copy(tokens[m], near.at[2 * m], sem_near.at[2 + m])

    def meta_send(dx, other):
        back = (4 - dx) % 4
        slot = back * 2 + other
        return remote(meta.at[0], meta.at[slot], sem_meta_send.at[dx * 2 + other], sem_meta_recv.at[slot], on_x(dx, other))

    others = [(dx, other) for dx in range(4) for other in range(2) if (dx, other) != (0, 0)]

    mine = lax.rem(y, 2) == core
    own_slot = z * 2 + y // 2

    def shard_y(k):
        return remote(shard_vmem, gath_hbm.at[own_slot], sem_sh_send.at[k], sem_sh_recv.at[own_slot], on_y((1, 3, 2)[k]))

    shard_in = [pltpu.make_async_copy(w, shard_vmem.at[i], sem_sh_own.at[i]) for i, w in enumerate((shared_w1, shared_w3, shared_w2))]
    shard_own = pltpu.make_async_copy(shard_vmem, gath_hbm.at[own_slot], sem_sh_own.at[3])

    def shard_wait(slot):
        pltpu.make_async_copy(shard_vmem, gath_hbm.at[slot], sem_sh_recv.at[slot]).wait()

    def shard_z(k):
        slot = z * 2 + k % 2
        return remote(gath_hbm.at[slot], gath_hbm.at[slot], sem_sh_send.at[3 + k], sem_sh_recv.at[slot], on_z((1, 3)[k // 2]))

    def shard_relay(k):
        slot = lax.rem(z + (3, 1)[k], 4) * 2 + k
        return remote(gath_hbm.at[slot], gath_hbm.at[slot], sem_sh_send.at[7 + k], sem_sh_recv.at[slot], on_z((1, 3)[k]))

    def weights_in(buf, expert, act):
        act(pltpu.make_async_copy(routed_w1.at[expert], w1.at[buf], sem_w.at[buf, 0]))
        act(pltpu.make_async_copy(routed_w3.at[expert], w3.at[buf], sem_w.at[buf, 1]))

    def weights_out(buf, expert, act):
        act(pltpu.make_async_copy(routed_w2.at[expert], w2.at[buf], sem_w.at[buf, 2]))

    def pair_copy(n):
        k = lax.rem(n, 2)
        return remote(pair_out.at[k], pair_in.at[k], sem_pair_send.at[n], sem_pair_recv.at[n], on_x(0, 1))

    def rs_turn(m, k):
        part, step, dst = ((low, 1, turn_p), (high, 3, turn_m))[k]
        return remote(sums.at[m, 0, part], dst.at[m], sem_rs_send.at[m, k], sem_rs_recv.at[m, k], on_x(step))

    def rs_last(m, k):
        part, step, dst, i = ((high, 1, last_m, 1), (low, 3, last_p, 2), (low, 1, last_m, 1), (high, 3, last_p, 2))[k]
        return remote(sums.at[m, i, part], dst.at[m, part], sem_rs_send.at[m, 2 + k], sem_rs_recv.at[m, 2 + k], on_x(step))

    def hits_of(slot, m):
        ids = meta[slot, 2 * m] - (ep * num_rows).astype(F32)
        row = lax.broadcasted_iota(jnp.int32, (num_rows, tok), 0).astype(F32)
        return [row == ids[j:j + 1, :] for j in range(top_k)]

    def place(q, slot, m, src, src_index):
        hits = hits_of(slot, m)
        matrix = functools.reduce(jnp.logical_or, hits)
        matrix = jnp.where(matrix, 1.0, 0.0).astype(BF16)
        for n in range(n_tiles):
            col = pl.ds(n * tile, tile)
            picked = jnp.dot(matrix, src[src_index, :, col], preferred_element_type=F32).astype(BF16)
            rows[:, q, :, col] = picked.reshape(local_experts, cap, tile)

    def ffn(expert, count, q0, nq, first=True, last=True):
        buf = lax.rem(count, 2)
        if first:
            weights_in(buf, expert, lambda c: c.wait())
        size = nq * cap
        x = rows[expert, pl.ds(q0, nq)].reshape(size, model_dim)
        for j in range(f_tiles):
            col = pl.ds(128 * j, 128)
            weight = jnp.concatenate([w1[buf, :, col], w3[buf, :, col]], axis=1)
            both = jnp.dot(x, weight, preferred_element_type=F32)
            hid[pl.ds(0, size), col] = (jax.nn.silu(both[:, :128]) * both[:, 128:]).astype(BF16)

        @pl.when(jnp.logical_and(last, count + 2 < 3 * local_experts))
        def _():
            weights_in(buf, lax.rem(expert + 2, local_experts), lambda c: c.start())

        if first:
            weights_out(buf, expert, lambda c: c.wait())
        h = hid[pl.ds(0, size), :]
        for n in range(n_tiles):
            col = pl.ds(n * tile, tile)
            res = jnp.dot(h, w2[buf, :, col], preferred_element_type=F32).astype(BF16)
            rows[expert, pl.ds(q0, nq), :, col] = res.reshape(nq, cap, tile)

        @pl.when(jnp.logical_and(last, count + 2 < 3 * local_experts))
        def _():
            weights_out(buf, lax.rem(expert + 2, local_experts), lambda c: c.start())

    def combine(q, slot, m, dst, add):
        gates = meta[slot, 2 * m + 1]
        matrix = 0.0
        for j, hit in enumerate(hits_of(slot, m)):
            matrix = matrix + jnp.where(hit, gates[j:j + 1, :], 0.0)
        matrix = jnp.concatenate(_split_gate(matrix), axis=0)
        for n in range(n_tiles):
            col = pl.ds(n * tile, tile)
            res = rows[:, q, :, col].reshape(num_rows, tile)
            res = jnp.concatenate([res, res, res], axis=0)
            part = lax.dot_general(matrix, res, (((0,), (0,)), ((), ())), preferred_element_type=F32)
            dst[:, col] = dst[:, col] + part if add else part

    def add_into(dst, src):
        step = min(32, dst.shape[0])

        def body(i, carry):
            part = pl.ds(pl.multiple_of(i * step, step), step)
            dst[part, :] = dst[part, :] + src[part, :]
            return carry
        lax.fori_loop(0, dst.shape[0] // step, body, 0)

    def shared_piece(p):
        return w1[p // f_tiles, pl.ds(0, ff), pl.ds(128 * (p % f_tiles), 128)]

    def shared(q, dst):
        x = near[q]
        width = min(tile, ff)
        dims = (((1,), (1,)), ((), ()))
        for start in range(0, ff, width):
            size = min(width, ff - start)
            row = pl.ds(start, size)
            a = lax.dot_general(x, w2[0, row, :], dims, preferred_element_type=F32)
            g = lax.dot_general(x, w2[1, row, :], dims, preferred_element_type=F32)
            hid[pl.ds(0, tok), row] = (jax.nn.silu(a) * g).astype(BF16)
        h = hid[pl.ds(0, tok), :]
        for n in range(n_tiles):
            weight = jnp.concatenate([shared_piece(2 * n), shared_piece(2 * n + 1)], axis=1)
            dst[:, pl.ds(n * tile, tile)] = jnp.dot(h, weight, preferred_element_type=F32)

    def shared_load(act):
        def body(k, carry):
            row = pl.ds(pl.multiple_of(k * shard, shard), shard)
            act(pltpu.make_async_copy(gath_hbm.at[k, 0], w2.at[0, row], sem_sh_load.at[k, 0]))
            act(pltpu.make_async_copy(gath_hbm.at[k, 1], w2.at[1, row], sem_sh_load.at[k, 1]))
            act(pltpu.make_async_copy(gath_hbm.at[k, 2, :, pl.ds(0, ff)], w1.at[0, row], sem_sh_load.at[k, 2]))
            rest = pl.ds(0, model_dim - ff)
            act(pltpu.make_async_copy(gath_hbm.at[k, 2, :, pl.ds(ff, model_dim - ff)], w1.at[1, row, rest], sem_sh_load.at[k, 3]))
            return carry
        lax.fori_loop(0, 8, body, 0)

    for i in range(2):
        weights_in(i, i, lambda c: c.start())
        weights_out(i, i, lambda c: c.start())
    near_own(0).start()
    near_own(1).start()
    for copy in shard_in:
        copy.start()
    for m, (experts, gates, slots) in enumerate(((exp_a, gate_a, slot_a), (exp_b, gate_b, slot_b))):
        meta[0, 2 * m] = jnp.zeros((8, tok), F32)
        meta[0, 2 * m + 1] = jnp.zeros((8, tok), F32)
        row = jnp.where(slots[...] >= 0, experts[...] * cap + slots[...], -1)
        meta[0, 2 * m, pl.ds(0, top_k), :] = row.astype(F32)
        meta[0, 2 * m + 1, pl.ds(0, top_k), :] = gates[...]
    barrier = pltpu.get_barrier_semaphore()
    peers = [on_x(dx, other) for dx, other in others] + [on_y(1), on_y(2), on_y(3), on_z(1), on_z(3)]
    for peer in peers:
        pl.semaphore_signal(barrier, inc=1, device_id=peer, device_id_type=MESH)
    pl.semaphore_wait(barrier, len(peers))

    for k in ORDER:
        ag_own(0, k).start()
    near_pair(0).start()
    near_pair(1).start()
    for dx, other in others:
        meta_send(dx, other).start()

    for copy in shard_in:
        copy.wait()

    @pl.when(mine)
    def _():
        for k in range(3):
            shard_y(k).start()
        shard_own.start()

    near_own(0).wait()
    near_own(1).wait()

    def place_near(i, carry):
        @pl.when(i == 2)
        def _():
            near_pair(0).wait_recv()
            near_pair(1).wait_recv()
            meta_send(0, 1).wait_recv()
        q = 2 * lax.rem(i, 2) + i // 2
        place(q, i // 2, lax.rem(i, 2), near, q)
        return carry
    lax.fori_loop(0, 4, place_near, 0)

    def ffn_near(e, carry):
        @pl.when(e == 2)
        def _():
            ag_own(0, 0).wait_recv()
            ag_relay(0, 0).start()
            ag_own(0, 2).wait_recv()
            ag_relay(0, 1).start()
            for k in ORDER:
                ag_own(1, k).start()

        @pl.when(e == 7)
        def _():
            ag_own(0, 1).wait_recv()
            ag_pair(0, 0).start()
            ag_own(0, 3).wait_recv()
            ag_pair(0, 1).start()
        ffn(e, e, 0, 4)
        return carry
    lax.fori_loop(0, local_experts, ffn_near, 0)

    for dx, other in others[1:]:
        meta_send(dx, other).wait_recv()

    def shards_on():
        for h in range(2):
            owned = jnp.logical_and(mine, y // 2 == h)

            @pl.when(owned)
            def _():
                shard_own.wait()

            @pl.when(jnp.logical_not(owned))
            def _():
                shard_wait(z * 2 + h)
        for k in range(4):
            shard_z(k).start()

    def turn(m):
        rs_turn(m, 0).wait_recv()
        add_into(sums.at[m, 1, low], turn_p.at[m])
        rs_last(m, 2).start()
        rs_turn(m, 1).wait_recv()
        add_into(sums.at[m, 2, high], turn_m.at[m])
        rs_last(m, 3).start()

    def far_slot(i):
        return jnp.where(i < 4, 2 + 4 * lax.rem(i, 2) + i // 2, i)

    def stage_copy(m, i):
        k = lax.rem(i, 4)
        return pltpu.make_async_copy(far_hbm.at[m, far_slot(i)], stage.at[k], sem_stage.at[k])

    def far_opposite(m):
        ag_relay(m, 0).wait_recv()
        ag_relay(m, 1).wait_recv()
        ag_pair(m, 2).start()

    def far(m, carry):
        def place_far(i, carry):
            stage_copy(m, i).wait()
            slot = far_slot(i)
            order = jnp.where(i < 4, 2 * lax.rem(i, 2) + i // 2, i)
            place(4 + 6 * m + order, slot, m, stage, lax.rem(i, 4))
            return carry

        stage_copy(m, 0).start()
        stage_copy(m, 1).start()
        ag_pair(m, 1).wait_recv()
        ag_pair(m, 0).wait_recv()
        stage_copy(m, 2).start()
        stage_copy(m, 3).start()
        lax.fori_loop(0, 4, place_far, 0)

        @pl.when(m == 0)
        def _():
            far_opposite(0)
        stage_copy(m, 4).start()
        ag_pair(m, 2).wait_recv()
        stage_copy(m, 5).start()
        lax.fori_loop(4, 6, place_far, 0)

        def ffn_far(e, carry):
            @pl.when(jnp.logical_and(m == 0, e == 0))
            def _():
                shards_on()

            @pl.when(jnp.logical_and(m == 0, e == 2))
            def _():
                ag_own(1, 0).wait_recv()
                ag_relay(1, 0).start()
                ag_own(1, 2).wait_recv()
                ag_relay(1, 1).start()

            @pl.when(jnp.logical_and(m == 0, e == 6))
            def _():
                ag_own(1, 1).wait_recv()
                ag_pair(1, 0).start()
                ag_own(1, 3).wait_recv()
                ag_pair(1, 1).start()

            @pl.when(jnp.logical_and(m == 0, e == 7))
            def _():
                far_opposite(1)

            @pl.when(jnp.logical_and(m == 1, e == 3))
            def _():
                turn(0)

            @pl.when(jnp.logical_and(m == 1, e == 6))
            def _():
                for step in (1, 3):
                    for h in range(2):
                        shard_wait(lax.rem(z + step, 4) * 2 + h)
                for k in range(2):
                    shard_relay(k).start()
            ffn(e, local_experts * (1 + m) + e, 4 + 6 * m, 6)
            return carry
        lax.fori_loop(0, local_experts, ffn_far, 0)

        slots, orders = (4, 2, 6), (4, 0, 2)

        def other(i):
            n = 3 * m + i
            k = lax.rem(n, 2)

            @pl.when(n >= 2)
            def _():
                pair_copy(n - 2).wait_send()
            combine(4 + 6 * m + orders[i] + 1, slots[i] + 1, m, pair_out.at[k], False)

            @pl.when(n >= 2)
            def _():
                pl.semaphore_wait(pair_free, 1)
            pair_copy(n).start()

        def same(i):
            combine(4 + 6 * m + orders[i], slots[i], m, sums.at[m, i], False)

        def complete(i):
            n = 3 * m + i
            pair_copy(n).wait_recv()
            add_into(sums.at[m, i], pair_in.at[lax.rem(n, 2)])
            pl.semaphore_signal(pair_free, inc=1, device_id=on_x(0, 1), device_id_type=MESH)
            if i == 0:
                rs_turn(m, 0).start()
                rs_turn(m, 1).start()
            else:
                rs_last(m, i - 1).start()

        other(0)
        other(1)
        same(0)
        complete(0)
        other(2)
        same(1)
        complete(1)
        same(2)
        complete(2)
        return carry

    lax.fori_loop(0, 2, far, 0)

    for h in range(2):
        shard_wait(lax.rem(z + 2, 4) * 2 + h)
    shared_load(lambda c: c.start())
    shared_load(lambda c: c.wait())

    def finish(m, carry):
        n = 6 + m
        k = lax.rem(n, 2)
        pair_copy(n - 2).wait_send()
        shared(2 * m + 1, pair_out.at[k])
        combine(2 * m + 1, 1, m, pair_out.at[k], True)
        pl.semaphore_wait(pair_free, 1)
        pair_copy(n).start()
        shared(2 * m, sums.at[m, 3])
        combine(2 * m, 0, m, sums.at[m, 3], True)

        @pl.when(m == 0)
        def _():
            turn(1)
        pair_copy(n).wait_recv()
        add_into(sums.at[m, 3], pair_in.at[k])
        return carry
    lax.fori_loop(0, 2, finish, 0)

    def out_copy(m, k):
        part = (low, high)[k]
        return pltpu.make_async_copy(near.at[2 * m, part], (out_a, out_b)[m].at[part], sem_out.at[m, k])

    step = min(32, half)
    for m in range(2):
        for k in ORDER:
            rs_last(m, k).wait_recv()

        def write(i, carry):
            part = pl.ds(pl.multiple_of(i * step, step), step)
            total = near[2 * m, part, :].astype(F32) + sums[m, 3, part, :]
            near[2 * m, part, :] = (total + last_p[m, part, :] + last_m[m, part, :]).astype(BF16)
            return carry
        for k in range(2):
            lax.fori_loop(k * half // step, (k + 1) * half // step, write, 0)
            out_copy(m, k).start()

    for m in range(2):
        for k in range(2):
            out_copy(m, k).wait()
        for k in range(4):
            ag_own(m, k).wait_send()
            rs_last(m, k).wait_send()
        for k in range(2):
            ag_relay(m, k).wait_send()
            rs_turn(m, k).wait_send()
        for k in range(3):
            ag_pair(m, k).wait_send()
        near_pair(m).wait_send()
        pair_copy(6 + m).wait_send()
    for dx, other in others:
        meta_send(dx, other).wait_send()

    @pl.when(mine)
    def _():
        for k in range(3):
            shard_y(k).wait_send()
    for k in range(4):
        shard_z(k).wait_send()
    for k in range(2):
        shard_relay(k).wait_send()


def _move_kernel(in_a, in_b, out_a, out_b, held, sem):
    half = in_a.shape[0] // 2
    copies = []
    for m, (src, dst) in enumerate(((in_a, out_a), (in_b, out_b))):
        for k in range(2):
            part = pl.ds(k * half, half)
            copies.append((
                pltpu.make_async_copy(src.at[part], held.at[m, part], sem.at[0, m, k]),
                pltpu.make_async_copy(held.at[m, part], dst.at[part], sem.at[1, m, k]),
            ))
    for fetch, _ in copies:
        fetch.start()
    for fetch, store in copies:
        fetch.wait()
        store.start()
    for _, store in copies:
        store.wait()


def solution(mesh):
    ep_size = mesh.shape['ep']
    tok_spec = P(('data', 'ep', 'tp'), None)
    columns, experts = P(None, 'tp'), P('ep', None, None)
    in_specs = (tok_spec,) * 8 + (columns, columns, P('tp', None), experts, experts, experts)

    def layer_local(tokens_a, tokens_b, experts_a, experts_b, gates_a, gates_b, slots_a, slots_b, shared_w1, shared_w3, shared_w2, routed_w1, routed_w3, routed_w2):
        tok, top_k = experts_a.shape
        local_experts, model_dim, ff = routed_w1.shape
        shard = shared_w2.shape[0]
        cap = max(4, (2 * tok * top_k) // (local_experts * ep_size))
        half = tok // 2

        hbm = pl.BlockSpec(memory_space=pl.ANY)
        dma = pltpu.SemaphoreType.DMA
        four, eight = dma((4,)), dma((8,))
        out_a, out_b, _, _ = pl.pallas_call(
            functools.partial(_layer_kernel, cap, top_k),
            out_shape=(
                jax.ShapeDtypeStruct((tok, model_dim), BF16),
                jax.ShapeDtypeStruct((tok, model_dim), BF16),
                jax.ShapeDtypeStruct((2, 8, tok, model_dim), BF16),
                jax.ShapeDtypeStruct((8, 3, shard, model_dim), BF16),
            ),
            in_specs=[hbm] * 2 + [pl.BlockSpec(memory_space=pltpu.VMEM)] * 6 + [hbm] * 6,
            out_specs=(hbm, hbm, hbm, hbm),
            scratch_shapes=[
                pltpu.VMEM((4, tok, model_dim), BF16),
                pltpu.VMEM((4, tok, model_dim), BF16),
                pltpu.VMEM((8, 4, 8, tok), F32),
                pltpu.VMEM((local_experts, 16, cap, model_dim), BF16),
                pltpu.VMEM((2, model_dim, ff), BF16),
                pltpu.VMEM((2, model_dim, ff), BF16),
                pltpu.VMEM((2, ff, model_dim), BF16),
                pltpu.VMEM((max(6 * cap, tok), ff), BF16),
                pltpu.VMEM((2, tok, model_dim), F32),
                pltpu.VMEM((2, tok, model_dim), F32),
                pltpu.VMEM((2, 4, tok, model_dim), F32),
                pltpu.VMEM((2, half, model_dim), F32),
                pltpu.VMEM((2, half, model_dim), F32),
                pltpu.VMEM((2, tok, model_dim), F32),
                pltpu.VMEM((2, tok, model_dim), F32),
                pltpu.VMEM((3, shard, model_dim), BF16),
                four, dma((2,)), eight, eight, *[dma((2, 9))] * 2, four, dma((2, 3)),
                dma((9,)), eight, four, dma((8, 4)), eight, eight, *[dma((2, 6))] * 2, dma((2, 2)),
                pltpu.SemaphoreType.REGULAR,
            ],
            compiler_params=pltpu.CompilerParams(collective_id=0, has_side_effects=True, vmem_limit_bytes=67_000_000),
        )(tokens_a, tokens_b, experts_a.T, experts_b.T, gates_a.T, gates_b.T, slots_a.T, slots_b.T, shared_w1.T, shared_w3.T, shared_w2, routed_w1, routed_w3, routed_w2)
        return pl.pallas_call(
            _move_kernel,
            out_shape=(jax.ShapeDtypeStruct((tok, model_dim), BF16),) * 2,
            in_specs=[hbm] * 2,
            out_specs=(hbm, hbm),
            scratch_shapes=[pltpu.VMEM((2, tok, model_dim), BF16), dma((2, 2, 2))],
            compiler_params=pltpu.CompilerParams(vmem_limit_bytes=66_000_000),
        )(out_a, out_b)

    return jax.shard_map(layer_local, mesh=mesh, in_specs=in_specs, out_specs=(tok_spec, tok_spec), check_vma=False)
```

```python
import functools

import jax
import jax.numpy as jnp
from jax import lax
from jax.experimental import pallas as pl
from jax.experimental.pallas import tpu as pltpu
from jax.sharding import PartitionSpec as P

MESH = pl.DeviceIdType.MESH
F32 = jnp.float32
BF16 = jnp.bfloat16
ORDER = (0, 2, 1, 3)


def _split_gate(gate):
    high = gate.astype(BF16)
    rest = gate - high.astype(F32)
    middle = rest.astype(BF16)
    low = (rest - middle.astype(F32)).astype(BF16)
    return high, middle, low


def _layer_kernel(
    cap, top_k,
    tok_a, tok_b, exp_a, exp_b, gate_a, gate_b, slot_a, slot_b, shared_w1, shared_w3, shared_w2, routed_w1, routed_w3, routed_w2,
    out_a, out_b, far_hbm, gath_hbm,
    near, stage, meta, rows, w1, w3, w2, hid, pair_out, pair_in, sums, turn_p, turn_m, last_p, last_m, shard_vmem,
    sem_near, sem_near_recv, sem_meta_send, sem_meta_recv, sem_ag_send, sem_ag_recv, sem_stage, sem_w,
    sem_sh_send, sem_sh_recv, sem_sh_own, sem_sh_load, sem_pair_send, sem_pair_recv, sem_rs_send, sem_rs_recv, sem_out, pair_free,
):
    local_experts, model_dim, ff = routed_w1.shape
    tok = tok_a.shape[0]
    half = tok // 2
    shard = shared_w2.shape[0]
    num_rows = local_experts * cap
    tile = 256
    n_tiles = model_dim // tile
    f_tiles = ff // 128

    ep = lax.axis_index('ep')
    tp = lax.axis_index('tp')
    chip, core = ep // 2, lax.rem(ep, 2)
    z, y = tp // 4, lax.rem(tp, 4)

    def on_x(step, other=0):
        side = core if other == 0 else 1 - core
        return {'ep': lax.rem(chip + step, 4) * 2 + side, 'tp': tp}

    def on_y(step):
        return {'ep': ep, 'tp': z * 4 + lax.rem(y + step, 4)}

    def on_z(step):
        return {'ep': ep, 'tp': lax.rem(z + step, 4) * 4 + y}

    def remote(src, dst, send, recv, device):
        return pltpu.make_async_remote_copy(src_ref=src, dst_ref=dst, send_sem=send, recv_sem=recv, device_id=device, device_id_type=MESH)

    low, high = pl.ds(0, half), pl.ds(half, half)

    tokens = (tok_a, tok_b)

    def ag_own(m, k):
        part, step, slot = ((low, 1, 6), (high, 1, 6), (high, 3, 2), (low, 3, 2))[k]
        return remote(tokens[m].at[part], far_hbm.at[m, slot, part], sem_ag_send.at[m, k], sem_ag_recv.at[m, k], on_x(step))

    def ag_relay(m, k):
        part, step, slot = ((low, 1, 6), (high, 3, 2))[k]
        return remote(far_hbm.at[m, slot, part], far_hbm.at[m, 4, part], sem_ag_send.at[m, 4 + k], sem_ag_recv.at[m, 4 + k], on_x(step))

    def ag_pair(m, k):
        slot = (6, 2, 4)[k]
        return remote(far_hbm.at[m, slot], far_hbm.at[m, slot + 1], sem_ag_send.at[m, 6 + k], sem_ag_recv.at[m, 6 + k], on_x(0, 1))

    def near_pair(m):
        return remote(tokens[m], near.at[2 * m + 1], sem_near.at[m], sem_near_recv.at[m], on_x(0, 1))

    def near_own(m):
        return pltpu.make_async_copy(tokens[m], near.at[2 * m], sem_near.at[2 + m])

    def meta_send(dx, other):
        back = (4 - dx) % 4
        slot = back * 2 + other
        return remote(meta.at[0], meta.at[slot], sem_meta_send.at[dx * 2 + other], sem_meta_recv.at[slot], on_x(dx, other))

    others = [(dx, other) for dx in range(4) for other in range(2) if (dx, other) != (0, 0)]

    mine = lax.rem(y, 2) == core
    own_slot = z * 2 + y // 2

    def shard_y(k):
        return remote(shard_vmem, gath_hbm.at[own_slot], sem_sh_send.at[k], sem_sh_recv.at[own_slot], on_y((1, 3, 2)[k]))

    shard_in = [pltpu.make_async_copy(w, shard_vmem.at[i], sem_sh_own.at[i]) for i, w in enumerate((shared_w1, shared_w3, shared_w2))]
    shard_own = pltpu.make_async_copy(shard_vmem, gath_hbm.at[own_slot], sem_sh_own.at[3])

    def shard_wait(slot):
        pltpu.make_async_copy(shard_vmem, gath_hbm.at[slot], sem_sh_recv.at[slot]).wait()

    def shard_z(k):
        slot = z * 2 + k % 2
        return remote(gath_hbm.at[slot], gath_hbm.at[slot], sem_sh_send.at[3 + k], sem_sh_recv.at[slot], on_z((1, 3)[k // 2]))

    def shard_relay(k):
        slot = lax.rem(z + (3, 1)[k], 4) * 2 + k
        return remote(gath_hbm.at[slot], gath_hbm.at[slot], sem_sh_send.at[7 + k], sem_sh_recv.at[slot], on_z((1, 3)[k]))

    def weights_in(buf, expert, act):
        act(pltpu.make_async_copy(routed_w1.at[expert], w1.at[buf], sem_w.at[buf, 0]))
        act(pltpu.make_async_copy(routed_w3.at[expert], w3.at[buf], sem_w.at[buf, 1]))

    def weights_out(buf, expert, act):
        act(pltpu.make_async_copy(routed_w2.at[expert], w2.at[buf], sem_w.at[buf, 2]))

    def pair_copy(n):
        k = lax.rem(n, 2)
        return remote(pair_out.at[k], pair_in.at[k], sem_pair_send.at[n], sem_pair_recv.at[n], on_x(0, 1))

    def rs_turn(m, k):
        part, step, dst = ((low, 1, turn_p), (high, 3, turn_m))[k]
        return remote(sums.at[m, 0, part], dst.at[m], sem_rs_send.at[m, k], sem_rs_recv.at[m, k], on_x(step))

    def rs_last(m, k):
        part, step, dst, i = ((high, 1, last_m, 1), (low, 3, last_p, 2), (low, 1, last_m, 1), (high, 3, last_p, 2))[k]
        return remote(sums.at[m, i, part], dst.at[m, part], sem_rs_send.at[m, 2 + k], sem_rs_recv.at[m, 2 + k], on_x(step))

    def hits_of(slot, m):
        ids = meta[slot, 2 * m] - (ep * num_rows).astype(F32)
        row = lax.broadcasted_iota(jnp.int32, (num_rows, tok), 0).astype(F32)
        return [row == ids[j:j + 1, :] for j in range(top_k)]

    def place(q, slot, m, src, src_index):
        hits = hits_of(slot, m)
        matrix = functools.reduce(jnp.logical_or, hits)
        matrix = jnp.where(matrix, 1.0, 0.0).astype(BF16)
        for n in range(n_tiles):
            col = pl.ds(n * tile, tile)
            picked = jnp.dot(matrix, src[src_index, :, col], preferred_element_type=F32).astype(BF16)
            rows[:, q, :, col] = picked.reshape(local_experts, cap, tile)

    def ffn(expert, count, q0, nq, first=True, last=True):
        buf = lax.rem(count, 2)
        if first:
            weights_in(buf, expert, lambda c: c.wait())
        size = nq * cap
        x = rows[expert, pl.ds(q0, nq)].reshape(size, model_dim)
        for j in range(f_tiles):
            col = pl.ds(128 * j, 128)
            weight = jnp.concatenate([w1[buf, :, col], w3[buf, :, col]], axis=1)
            both = jnp.dot(x, weight, preferred_element_type=F32)
            hid[pl.ds(0, size), col] = (jax.nn.silu(both[:, :128]) * both[:, 128:]).astype(BF16)

        @pl.when(jnp.logical_and(last, count + 2 < 3 * local_experts))
        def _():
            weights_in(buf, lax.rem(expert + 2, local_experts), lambda c: c.start())

        if first:
            weights_out(buf, expert, lambda c: c.wait())
        h = hid[pl.ds(0, size), :]
        for n in range(n_tiles):
            col = pl.ds(n * tile, tile)
            res = jnp.dot(h, w2[buf, :, col], preferred_element_type=F32).astype(BF16)
            rows[expert, pl.ds(q0, nq), :, col] = res.reshape(nq, cap, tile)

        @pl.when(jnp.logical_and(last, count + 2 < 3 * local_experts))
        def _():
            weights_out(buf, lax.rem(expert + 2, local_experts), lambda c: c.start())

    def combine(q, slot, m, dst, add):
        gates = meta[slot, 2 * m + 1]
        matrix = 0.0
        for j, hit in enumerate(hits_of(slot, m)):
            matrix = matrix + jnp.where(hit, gates[j:j + 1, :], 0.0)
        matrix = jnp.concatenate(_split_gate(matrix), axis=0)
        for n in range(n_tiles):
            col = pl.ds(n * tile, tile)
            res = rows[:, q, :, col].reshape(num_rows, tile)
            res = jnp.concatenate([res, res, res], axis=0)
            part = lax.dot_general(matrix, res, (((0,), (0,)), ((), ())), preferred_element_type=F32)
            dst[:, col] = dst[:, col] + part if add else part

    def add_into(dst, src):
        step = min(32, dst.shape[0])

        def body(i, carry):
            part = pl.ds(pl.multiple_of(i * step, step), step)
            dst[part, :] = dst[part, :] + src[part, :]
            return carry
        lax.fori_loop(0, dst.shape[0] // step, body, 0)

    def shared_piece(p):
        return w1[p // f_tiles, pl.ds(0, ff), pl.ds(128 * (p % f_tiles), 128)]

    def shared(q, dst):
        x = near[q]
        width = min(tile, ff)
        dims = (((1,), (1,)), ((), ()))
        for start in range(0, ff, width):
            size = min(width, ff - start)
            row = pl.ds(start, size)
            a = lax.dot_general(x, w2[0, row, :], dims, preferred_element_type=F32)
            g = lax.dot_general(x, w2[1, row, :], dims, preferred_element_type=F32)
            hid[pl.ds(0, tok), row] = (jax.nn.silu(a) * g).astype(BF16)
        h = hid[pl.ds(0, tok), :]
        for n in range(n_tiles):
            weight = jnp.concatenate([shared_piece(2 * n), shared_piece(2 * n + 1)], axis=1)
            dst[:, pl.ds(n * tile, tile)] = jnp.dot(h, weight, preferred_element_type=F32)

    def shared_load(act):
        def body(k, carry):
            row = pl.ds(pl.multiple_of(k * shard, shard), shard)
            act(pltpu.make_async_copy(gath_hbm.at[k, 0], w2.at[0, row], sem_sh_load.at[k, 0]))
            act(pltpu.make_async_copy(gath_hbm.at[k, 1], w2.at[1, row], sem_sh_load.at[k, 1]))
            act(pltpu.make_async_copy(gath_hbm.at[k, 2, :, pl.ds(0, ff)], w1.at[0, row], sem_sh_load.at[k, 2]))
            rest = pl.ds(0, model_dim - ff)
            act(pltpu.make_async_copy(gath_hbm.at[k, 2, :, pl.ds(ff, model_dim - ff)], w1.at[1, row, rest], sem_sh_load.at[k, 3]))
            return carry
        lax.fori_loop(0, 8, body, 0)

    for i in range(2):
        weights_in(i, i, lambda c: c.start())
        weights_out(i, i, lambda c: c.start())
    near_own(0).start()
    near_own(1).start()
    for copy in shard_in:
        copy.start()
    for m, (experts, gates, slots) in enumerate(((exp_a, gate_a, slot_a), (exp_b, gate_b, slot_b))):
        meta[0, 2 * m] = jnp.zeros((8, tok), F32)
        meta[0, 2 * m + 1] = jnp.zeros((8, tok), F32)
        row = jnp.where(slots[...] >= 0, experts[...] * cap + slots[...], -1)
        meta[0, 2 * m, pl.ds(0, top_k), :] = row.astype(F32)
        meta[0, 2 * m + 1, pl.ds(0, top_k), :] = gates[...]
    barrier = pltpu.get_barrier_semaphore()
    peers = [on_x(dx, other) for dx, other in others] + [on_y(1), on_y(2), on_y(3), on_z(1), on_z(3)]
    for peer in peers:
        pl.semaphore_signal(barrier, inc=1, device_id=peer, device_id_type=MESH)
    pl.semaphore_wait(barrier, len(peers))

    for k in ORDER:
        ag_own(0, k).start()
    near_pair(0).start()
    near_pair(1).start()
    for dx, other in others:
        meta_send(dx, other).start()

    for copy in shard_in:
        copy.wait()

    @pl.when(mine)
    def _():
        for k in range(3):
            shard_y(k).start()
        shard_own.start()

    near_own(0).wait()
    near_own(1).wait()

    def place_near(i, carry):
        @pl.when(i == 2)
        def _():
            near_pair(0).wait_recv()
            near_pair(1).wait_recv()
            meta_send(0, 1).wait_recv()
        q = 2 * lax.rem(i, 2) + i // 2
        place(q, i // 2, lax.rem(i, 2), near, q)
        return carry
    lax.fori_loop(0, 4, place_near, 0)

    def ffn_near(e, carry):
        @pl.when(e == 2)
        def _():
            ag_own(0, 0).wait_recv()
            ag_relay(0, 0).start()
            ag_own(0, 2).wait_recv()
            ag_relay(0, 1).start()
            for k in ORDER:
                ag_own(1, k).start()

        @pl.when(e == 6)
        def _():
            ag_own(0, 1).wait_recv()
            ag_pair(0, 0).start()
            ag_own(0, 3).wait_recv()
            ag_pair(0, 1).start()
        ffn(e, e, 0, 4)
        return carry
    lax.fori_loop(0, local_experts, ffn_near, 0)

    for dx, other in others[1:]:
        meta_send(dx, other).wait_recv()

    def shards_on():
        for h in range(2):
            owned = jnp.logical_and(mine, y // 2 == h)

            @pl.when(owned)
            def _():
                shard_own.wait()

            @pl.when(jnp.logical_not(owned))
            def _():
                shard_wait(z * 2 + h)
        for k in range(4):
            shard_z(k).start()

    def turn(m):
        rs_turn(m, 0).wait_recv()
        add_into(sums.at[m, 1, low], turn_p.at[m])
        rs_last(m, 2).start()
        rs_turn(m, 1).wait_recv()
        add_into(sums.at[m, 2, high], turn_m.at[m])
        rs_last(m, 3).start()

    def far_slot(i):
        return jnp.where(i < 4, 2 + 4 * lax.rem(i, 2) + i // 2, i)

    def stage_copy(m, i):
        k = lax.rem(i, 4)
        return pltpu.make_async_copy(far_hbm.at[m, far_slot(i)], stage.at[k], sem_stage.at[k])

    def far_opposite(m):
        ag_relay(m, 0).wait_recv()
        ag_relay(m, 1).wait_recv()
        ag_pair(m, 2).start()

    def far(m, carry):
        def place_far(i, carry):
            stage_copy(m, i).wait()
            slot = far_slot(i)
            order = jnp.where(i < 4, 2 * lax.rem(i, 2) + i // 2, i)
            place(4 + 6 * m + order, slot, m, stage, lax.rem(i, 4))
            return carry

        stage_copy(m, 0).start()
        stage_copy(m, 1).start()
        ag_pair(m, 1).wait_recv()
        ag_pair(m, 0).wait_recv()
        stage_copy(m, 2).start()
        stage_copy(m, 3).start()
        lax.fori_loop(0, 4, place_far, 0)

        @pl.when(m == 0)
        def _():
            far_opposite(0)
        stage_copy(m, 4).start()
        ag_pair(m, 2).wait_recv()
        stage_copy(m, 5).start()
        lax.fori_loop(4, 6, place_far, 0)

        def ffn_far(e, carry):
            @pl.when(jnp.logical_and(m == 0, e == 0))
            def _():
                shards_on()

            @pl.when(jnp.logical_and(m == 0, e == 2))
            def _():
                ag_own(1, 0).wait_recv()
                ag_relay(1, 0).start()
                ag_own(1, 2).wait_recv()
                ag_relay(1, 1).start()

            @pl.when(jnp.logical_and(m == 0, e == 6))
            def _():
                ag_own(1, 1).wait_recv()
                ag_pair(1, 0).start()
                ag_own(1, 3).wait_recv()
                ag_pair(1, 1).start()

            @pl.when(jnp.logical_and(m == 0, e == 7))
            def _():
                far_opposite(1)

            @pl.when(jnp.logical_and(m == 1, e == 4))
            def _():
                turn(0)

            @pl.when(jnp.logical_and(m == 1, e == 6))
            def _():
                for step in (1, 3):
                    for h in range(2):
                        shard_wait(lax.rem(z + step, 4) * 2 + h)
                for k in range(2):
                    shard_relay(k).start()
            ffn(e, local_experts * (1 + m) + e, 4 + 6 * m, 6)
            return carry
        lax.fori_loop(0, local_experts, ffn_far, 0)

        slots, orders = (4, 2, 6), (4, 0, 2)

        def other(i):
            n = 3 * m + i
            k = lax.rem(n, 2)

            @pl.when(n >= 2)
            def _():
                pair_copy(n - 2).wait_send()
            combine(4 + 6 * m + orders[i] + 1, slots[i] + 1, m, pair_out.at[k], False)

            @pl.when(n >= 2)
            def _():
                pl.semaphore_wait(pair_free, 1)
            pair_copy(n).start()

        def same(i):
            combine(4 + 6 * m + orders[i], slots[i], m, sums.at[m, i], False)

        def complete(i):
            n = 3 * m + i
            pair_copy(n).wait_recv()
            add_into(sums.at[m, i], pair_in.at[lax.rem(n, 2)])
            pl.semaphore_signal(pair_free, inc=1, device_id=on_x(0, 1), device_id_type=MESH)
            if i == 0:
                rs_turn(m, 0).start()
                rs_turn(m, 1).start()
            else:
                rs_last(m, i - 1).start()

        other(0)
        other(1)
        same(0)
        complete(0)
        other(2)
        same(1)
        complete(1)
        same(2)
        complete(2)
        return carry

    lax.fori_loop(0, 2, far, 0)

    for h in range(2):
        shard_wait(lax.rem(z + 2, 4) * 2 + h)
    shared_load(lambda c: c.start())
    shared_load(lambda c: c.wait())

    def finish(m, carry):
        n = 6 + m
        k = lax.rem(n, 2)
        pair_copy(n - 2).wait_send()
        shared(2 * m + 1, pair_out.at[k])
        combine(2 * m + 1, 1, m, pair_out.at[k], True)
        pl.semaphore_wait(pair_free, 1)
        pair_copy(n).start()
        shared(2 * m, sums.at[m, 3])
        combine(2 * m, 0, m, sums.at[m, 3], True)

        @pl.when(m == 0)
        def _():
            turn(1)
        pair_copy(n).wait_recv()
        add_into(sums.at[m, 3], pair_in.at[k])
        return carry
    lax.fori_loop(0, 2, finish, 0)

    def out_copy(m, k):
        part = (low, high)[k]
        return pltpu.make_async_copy(near.at[2 * m, part], (out_a, out_b)[m].at[part], sem_out.at[m, k])

    step = min(32, half)
    for m in range(2):
        for k in ORDER:
            rs_last(m, k).wait_recv()

        def write(i, carry):
            part = pl.ds(pl.multiple_of(i * step, step), step)
            total = near[2 * m, part, :].astype(F32) + sums[m, 3, part, :]
            near[2 * m, part, :] = (total + last_p[m, part, :] + last_m[m, part, :]).astype(BF16)
            return carry
        for k in range(2):
            lax.fori_loop(k * half // step, (k + 1) * half // step, write, 0)
            out_copy(m, k).start()

    for m in range(2):
        for k in range(2):
            out_copy(m, k).wait()
        for k in range(4):
            ag_own(m, k).wait_send()
            rs_last(m, k).wait_send()
        for k in range(2):
            ag_relay(m, k).wait_send()
            rs_turn(m, k).wait_send()
        for k in range(3):
            ag_pair(m, k).wait_send()
        near_pair(m).wait_send()
        pair_copy(6 + m).wait_send()
    for dx, other in others:
        meta_send(dx, other).wait_send()

    @pl.when(mine)
    def _():
        for k in range(3):
            shard_y(k).wait_send()
    for k in range(4):
        shard_z(k).wait_send()
    for k in range(2):
        shard_relay(k).wait_send()


def _move_kernel(in_a, in_b, out_a, out_b, held, sem):
    half = in_a.shape[0] // 2
    copies = []
    for m, (src, dst) in enumerate(((in_a, out_a), (in_b, out_b))):
        for k in range(2):
            part = pl.ds(k * half, half)
            copies.append((
                pltpu.make_async_copy(src.at[part], held.at[m, part], sem.at[0, m, k]),
                pltpu.make_async_copy(held.at[m, part], dst.at[part], sem.at[1, m, k]),
            ))
    for fetch, _ in copies:
        fetch.start()
    for fetch, store in copies:
        fetch.wait()
        store.start()
    for _, store in copies:
        store.wait()


def solution(mesh):
    ep_size = mesh.shape['ep']
    tok_spec = P(('data', 'ep', 'tp'), None)
    columns, experts = P(None, 'tp'), P('ep', None, None)
    in_specs = (tok_spec,) * 8 + (columns, columns, P('tp', None), experts, experts, experts)

    def layer_local(tokens_a, tokens_b, experts_a, experts_b, gates_a, gates_b, slots_a, slots_b, shared_w1, shared_w3, shared_w2, routed_w1, routed_w3, routed_w2):
        tok, top_k = experts_a.shape
        local_experts, model_dim, ff = routed_w1.shape
        shard = shared_w2.shape[0]
        cap = max(4, (2 * tok * top_k) // (local_experts * ep_size))
        half = tok // 2

        hbm = pl.BlockSpec(memory_space=pl.ANY)
        dma = pltpu.SemaphoreType.DMA
        four, eight = dma((4,)), dma((8,))
        out_a, out_b, _, _ = pl.pallas_call(
            functools.partial(_layer_kernel, cap, top_k),
            out_shape=(
                jax.ShapeDtypeStruct((tok, model_dim), BF16),
                jax.ShapeDtypeStruct((tok, model_dim), BF16),
                jax.ShapeDtypeStruct((2, 8, tok, model_dim), BF16),
                jax.ShapeDtypeStruct((8, 3, shard, model_dim), BF16),
            ),
            in_specs=[hbm] * 2 + [pl.BlockSpec(memory_space=pltpu.VMEM)] * 6 + [hbm] * 6,
            out_specs=(hbm, hbm, hbm, hbm),
            scratch_shapes=[
                pltpu.VMEM((4, tok, model_dim), BF16),
                pltpu.VMEM((4, tok, model_dim), BF16),
                pltpu.VMEM((8, 4, 8, tok), F32),
                pltpu.VMEM((local_experts, 16, cap, model_dim), BF16),
                pltpu.VMEM((2, model_dim, ff), BF16),
                pltpu.VMEM((2, model_dim, ff), BF16),
                pltpu.VMEM((2, ff, model_dim), BF16),
                pltpu.VMEM((max(6 * cap, tok), ff), BF16),
                pltpu.VMEM((2, tok, model_dim), F32),
                pltpu.VMEM((2, tok, model_dim), F32),
                pltpu.VMEM((2, 4, tok, model_dim), F32),
                pltpu.VMEM((2, half, model_dim), F32),
                pltpu.VMEM((2, half, model_dim), F32),
                pltpu.VMEM((2, tok, model_dim), F32),
                pltpu.VMEM((2, tok, model_dim), F32),
                pltpu.VMEM((3, shard, model_dim), BF16),
                four, dma((2,)), eight, eight, *[dma((2, 9))] * 2, four, dma((2, 3)),
                dma((9,)), eight, four, dma((8, 4)), eight, eight, *[dma((2, 6))] * 2, dma((2, 2)),
                pltpu.SemaphoreType.REGULAR,
            ],
            compiler_params=pltpu.CompilerParams(collective_id=0, has_side_effects=True, vmem_limit_bytes=67_000_000),
        )(tokens_a, tokens_b, experts_a.T, experts_b.T, gates_a.T, gates_b.T, slots_a.T, slots_b.T, shared_w1.T, shared_w3.T, shared_w2, routed_w1, routed_w3, routed_w2)
        return pl.pallas_call(
            _move_kernel,
            out_shape=(jax.ShapeDtypeStruct((tok, model_dim), BF16),) * 2,
            in_specs=[hbm] * 2,
            out_specs=(hbm, hbm),
            scratch_shapes=[pltpu.VMEM((2, tok, model_dim), BF16), dma((2, 2, 2))],
            compiler_params=pltpu.CompilerParams(vmem_limit_bytes=66_000_000),
        )(out_a, out_b)

    return jax.shard_map(layer_local, mesh=mesh, in_specs=in_specs, out_specs=(tok_spec, tok_spec), check_vma=False)
```
